16 devices in a mesh: dp: 4 (over z, y), tp: 4 (over x, core).
Axes of the slice: x: 2, y: 2, z: 2, core: 2. Of those that a mesh axis runs over, the one named last changes fastest.
Arguments:
- y_one: float32 [16, 64, 2048], P('dp', 'tp'), parts along dimension 0
- y_two: float32 [16, 64, 2048], P('dp', 'tp'), parts along dimension 0
- dy_one: float32 [16, 64, 2048], P('dp', 'tp'), parts along dimension 0
- dy_two: float32 [16, 64, 2048], P('dp', 'tp'), parts along dimension 0
- w_qkv: bfloat16 [1, 2048, 32, 3, 64], P(None, None, 'tp')
- w_out: bfloat16 [1, 32, 64, 2048], P(None, 'tp')
- w_up: bfloat16 [1, 2048, 8192], P(None, None, 'tp')
- w_down: bfloat16 [1, 8192, 2048], P(None, 'tp')
Outputs:
- output 1: float32 [16, 64, 2048], P('dp', 'tp'), parts along dimension 0
- output 2: float32 [16, 64, 2048], P('dp', 'tp'), parts along dimension 0
- output 3: float32 [16, 64, 2048], P('dp', 'tp'), parts along dimension 0
- output 4: float32 [16, 64, 2048], P('dp', 'tp'), parts along dimension 0
- output 5: float32 [4, 2048, 32, 3, 64], P('dp', None, 'tp'), parts along dimension 0
- output 6: float32 [4, 32, 64, 2048], P('dp', 'tp'), parts along dimension 0
- output 7: float32 [4, 2048, 8192], P('dp', None, 'tp'), parts along dimension 0
- output 8: float32 [4, 8192, 2048], P('dp', 'tp'), parts along dimension 0
There are 4 independent parts. The reference program is written for one: setup_inputs(seed, part) draws one part's arguments, and reference() takes and returns one part's arrays. A program takes and returns all parts, laid end to end along the dimension named above; an argument that names none is the same for every part.
All inputs are finite; a program needn't handle non-finite values.
Results may differ from the reference program's by a relative error of at most 0.00900579.
Values are sent between devices in bfloat16 or wider.
A program may use at most 1 GiB of HBM per device.

```python
import jax
import jax.numpy as jnp
from jax import lax

SEQ_COUNT = 4
SEQ_LEN = 64
HIDDEN = 2048
N_HEADS = 32
FFN_DIM = 8192
N_LAYERS = 1

HEAD_DIM = HIDDEN // N_HEADS
TOKENS = SEQ_COUNT * SEQ_LEN
STATE_SHAPE = (SEQ_COUNT, SEQ_LEN, HIDDEN)
RMS_EPS = 1e-6
ATTN_SCALE = HEAD_DIM ** -0.5
Q_GAIN = 2.5
OUT_GAIN = 0.6
DOWN_GAIN = 0.5


def setup_inputs(seed: int = 0, part: int = 0) -> dict:
    base_key = jax.random.key(seed)
    act_keys = jax.random.split(jax.random.fold_in(base_key, part), 4)
    w_keys = jax.random.split(jax.random.fold_in(base_key, 100003), 4)
    y_one = jax.random.normal(act_keys[0], STATE_SHAPE, jnp.float32)
    y_two = jax.random.normal(act_keys[1], STATE_SHAPE, jnp.float32)
    dy_one = jax.random.normal(act_keys[2], STATE_SHAPE, jnp.float32)
    dy_two = jax.random.normal(act_keys[3], STATE_SHAPE, jnp.float32)
    qkv_gain = jnp.array([Q_GAIN, 1.0, 1.0], jnp.float32).reshape(1, 1, 1, 3, 1)
    w_qkv = (jax.random.normal(w_keys[0], (N_LAYERS, HIDDEN, N_HEADS, 3, HEAD_DIM), jnp.float32) * qkv_gain * HIDDEN ** -0.5).astype(jnp.bfloat16)
    w_out = (jax.random.normal(w_keys[1], (N_LAYERS, N_HEADS, HEAD_DIM, HIDDEN), jnp.float32) * (OUT_GAIN * HIDDEN ** -0.5)).astype(jnp.bfloat16)
    w_up = (jax.random.normal(w_keys[2], (N_LAYERS, HIDDEN, FFN_DIM), jnp.float32) * HIDDEN ** -0.5).astype(jnp.bfloat16)
    w_down = (jax.random.normal(w_keys[3], (N_LAYERS, FFN_DIM, HIDDEN), jnp.float32) * (DOWN_GAIN * FFN_DIM ** -0.5)).astype(jnp.bfloat16)
    return {"y_one": y_one, "y_two": y_two, "dy_one": dy_one, "dy_two": dy_two, "w_qkv": w_qkv, "w_out": w_out, "w_up": w_up, "w_down": w_down}


def rms_norm(tensor):
    return tensor * lax.rsqrt(jnp.mean(tensor * tensor, axis=-1, keepdims=True) + RMS_EPS)


def rms_back(tensor, grad_in):
    inv_rms = lax.rsqrt(jnp.mean(tensor * tensor, axis=-1, keepdims=True) + RMS_EPS)
    return inv_rms * grad_in - tensor * (inv_rms * inv_rms * inv_rms) * jnp.mean(grad_in * tensor, axis=-1, keepdims=True)


def gelu_tanh(tensor):
    return jax.nn.gelu(tensor, approximate=True)


def mixed_dot(left, right):
    return jnp.dot(left, right, preferred_element_type=jnp.float32)


def as_wide(tensor):
    return tensor.astype(jnp.float32)


def attn_forward(qkv_seq):
    q_heads = as_wide(qkv_seq[0])
    k_heads = as_wide(qkv_seq[1])
    v_heads = as_wide(qkv_seq[2])
    scores = jnp.einsum("nqd,nkd->nqk", q_heads, k_heads) * ATTN_SCALE
    attn_prob = jax.nn.softmax(scores, axis=-1)
    context = jnp.einsum("nqk,nkd->nqd", as_wide(attn_prob.astype(jnp.bfloat16)), v_heads)
    return context.astype(jnp.bfloat16)


def attn_backward(operands):
    qkv_seq, d_context = operands
    q_heads = as_wide(qkv_seq[0])
    k_heads = as_wide(qkv_seq[1])
    v_heads = as_wide(qkv_seq[2])
    scores = jnp.einsum("nqd,nkd->nqk", q_heads, k_heads) * ATTN_SCALE
    attn_prob = jax.nn.softmax(scores, axis=-1)
    d_ctx = as_wide(d_context)
    d_prob = jnp.einsum("nqd,nkd->nqk", d_ctx, v_heads)
    d_value = jnp.einsum("nqk,nqd->nkd", as_wide(attn_prob.astype(jnp.bfloat16)), d_ctx)
    d_scores = attn_prob * (d_prob - jnp.sum(d_prob * attn_prob, axis=-1, keepdims=True)) * ATTN_SCALE
    d_scores = as_wide(d_scores.astype(jnp.bfloat16))
    d_query = jnp.einsum("nqk,nkd->nqd", d_scores, k_heads)
    d_key = jnp.einsum("nqk,nqd->nkd", d_scores, q_heads)
    return jnp.stack([d_query, d_key, d_value]).astype(jnp.bfloat16)


def block_backward(state_in, layer_weights):
    y_one, y_two, dy_one, dy_two = state_in
    w_qkv, w_out, w_up, w_down = layer_weights
    w_qkv_flat = w_qkv.reshape(HIDDEN, 3 * HIDDEN)
    w_out_flat = w_out.reshape(HIDDEN, HIDDEN)
    u_mlp = rms_norm(y_one).astype(jnp.bfloat16).reshape(TOKENS, HIDDEN)
    pre_act = mixed_dot(u_mlp, w_up)
    hidden, gelu_pull = jax.vjp(gelu_tanh, pre_act)
    hidden_b = hidden.astype(jnp.bfloat16)
    x_two = y_two - mixed_dot(hidden_b, w_down).reshape(STATE_SHAPE)
    cot_mlp = dy_two.astype(jnp.bfloat16).reshape(TOKENS, HIDDEN)
    dw_down = mixed_dot(hidden_b.T, cot_mlp)
    d_pre = gelu_pull(mixed_dot(cot_mlp, w_down.T))[0].astype(jnp.bfloat16)
    dw_up = mixed_dot(u_mlp.T, d_pre)
    dy_one = dy_one + rms_back(y_one, mixed_dot(d_pre, w_up.T).reshape(STATE_SHAPE))
    u_att = rms_norm(x_two).astype(jnp.bfloat16).reshape(TOKENS, HIDDEN)
    qkv_seqs = mixed_dot(u_att, w_qkv_flat).astype(jnp.bfloat16).reshape(SEQ_COUNT, SEQ_LEN, N_HEADS, 3, HEAD_DIM).transpose(0, 3, 2, 1, 4)
    context = lax.map(attn_forward, qkv_seqs)
    context_flat = context.transpose(0, 2, 1, 3).reshape(TOKENS, HIDDEN)
    x_one = y_one - mixed_dot(context_flat, w_out_flat).reshape(STATE_SHAPE)
    cot_att = dy_one.astype(jnp.bfloat16).reshape(TOKENS, HIDDEN)
    dw_out = mixed_dot(context_flat.T, cot_att)
    d_context = mixed_dot(cot_att, w_out_flat.T).astype(jnp.bfloat16).reshape(SEQ_COUNT, SEQ_LEN, N_HEADS, HEAD_DIM).transpose(0, 2, 1, 3)
    d_qkv = lax.map(attn_backward, (qkv_seqs, d_context))
    d_qkv_flat = d_qkv.transpose(0, 3, 2, 1, 4).reshape(TOKENS, 3 * HIDDEN)
    dw_qkv = mixed_dot(u_att.T, d_qkv_flat)
    dx_two = dy_two + rms_back(x_two, mixed_dot(d_qkv_flat, w_qkv_flat.T).reshape(STATE_SHAPE))
    grads = (dw_qkv.reshape(HIDDEN, N_HEADS, 3, HEAD_DIM), dw_out.reshape(N_HEADS, HEAD_DIM, HIDDEN), dw_up, dw_down)
    return (x_one, x_two, dy_one, dx_two), grads


def reference(y_one, y_two, dy_one, dy_two, w_qkv, w_out, w_up, w_down):
    final_state, grad_stack = lax.scan(block_backward, (y_one, y_two, dy_one, dy_two), (w_qkv, w_out, w_up, w_down), reverse=True)
    x_one, x_two, dx_one, dx_two = final_state
    dw_qkv, dw_out, dw_up, dw_down = grad_stack
    return (x_one, x_two, dx_one, dx_two, dw_qkv, dw_out, dw_up, dw_down)
```

```python
import functools

import jax
import jax.numpy as jnp
from jax import lax
from jax.experimental import pallas as pl
from jax.experimental.pallas import tpu as pltpu
from jax.sharding import PartitionSpec as P


EPS = 1e-6
F32, BF16 = jnp.float32, jnp.bfloat16
MIB = 1 << 20
WHOLE = pl.BlockSpec(memory_space=pltpu.VMEM)
ANY = pl.BlockSpec(memory_space=pl.ANY)
GELU_A = 0.7978845608028654
GELU_B = 0.044715


def nn(left, right):
    return lax.dot_general(left, right, (((1,), (0,)), ((), ())), preferred_element_type=F32)


def nt(left, right):
    return lax.dot_general(left, right, (((1,), (1,)), ((), ())), preferred_element_type=F32)


def tn(left, right):
    return lax.dot_general(left, right, (((0,), (0,)), ((), ())), preferred_element_type=F32)


def rows(*refs):
    return jnp.concatenate([r[...] for r in refs], axis=0)


def sds(shape, dtype):
    return jax.ShapeDtypeStruct(shape, dtype)


def call(body, out_shape, args, *, vmem, flops, name, **kw):
    nbytes = sum(a.size * a.dtype.itemsize for a in args)
    return pl.pallas_call(
        body,
        out_shape=out_shape,
        name=name,
        compiler_params=pltpu.CompilerParams(vmem_limit_bytes=vmem * MIB),
        cost_estimate=pl.CostEstimate(flops=int(flops), bytes_accessed=int(nbytes), transcendentals=0),
        **kw,
    )(*args)


def inv_rms(x):
    return lax.rsqrt(jnp.mean(x * x, axis=-1, keepdims=True) + EPS)


def norm_back(x, g):
    inv = inv_rms(x)
    return inv * g - x * (inv * inv * inv) * jnp.mean(g * x, axis=-1, keepdims=True)


def gelu_pair(a):
    sq = a * a
    t = jnp.tanh(GELU_A * (a + GELU_B * (sq * a)))
    cdf = 0.5 * (1.0 + t)
    slope = cdf + (0.5 * a) * (1.0 - t * t) * (GELU_A * (1.0 + (3.0 * GELU_B) * sq))
    return a * cdf, slope


def norm_body(y, u):
    u[...] = (y[...] * inv_rms(y[...])).astype(BF16)


def cast_body(y, c):
    c[...] = y[...].astype(BF16)


def x2_body(y2, own, near, far0, far1, x2, u):
    far = jnp.concatenate([far0[...], far1[...]], axis=1)
    x = y2[...] - (own[...] + near[...] + far)
    x2[...] = x
    u[...] = (x * inv_rms(x)).astype(BF16)


def dy_body(x, dy, own, near, far0, far1, out, c):
    far = jnp.concatenate([far0[...], far1[...]], axis=1)
    new = dy[...] + norm_back(x[...], own[...] + near[...] + far)
    out[...] = new
    c[...] = new.astype(BF16)


def dx_body(x, dy, own, near, far0, far1, out):
    far = jnp.concatenate([far0[...], far1[...]], axis=1)
    out[...] = dy[...] + norm_back(x[...], own[...] + near[...] + far)


def sub_body(y, own, near, far0, far1, out):
    far = jnp.concatenate([far0[...], far1[...]], axis=1)
    out[...] = y[...] - (own[...] + near[...] + far)


def add_body(left, right, out):
    out[...] = left[...] + right[...]


FB = 256


def mlp_near_body(u0, u1, c0, c1, w1, w2, h, da, g0, g1, d0, d1, w1v, w2v, s1, s2):
    n_blk = w1v.shape[1] // FB
    half = u0.shape[0]

    def block(i):
        return pl.ds(pl.multiple_of(i * FB, FB), FB)

    def copies(i):
        return (
            pltpu.make_async_copy(w1.at[:, block(i)], w1v.at[:, block(i)], s1.at[i]),
            pltpu.make_async_copy(w2.at[block(i)], w2v.at[block(i)], s2.at[i]),
        )

    for i in range(n_blk):
        for c in copies(i):
            c.start()
    for ref in (g0, g1, d0, d1):
        ref[...] = jnp.zeros_like(ref)

    @pl.loop(0, n_blk)
    def _(i):
        for c in copies(i):
            c.wait()
        blk = block(i)
        a = nn(rows(u0, u1), w1v[:, blk])
        hid, slope = gelu_pair(a)
        hid = hid.astype(BF16)
        h[:, blk] = hid
        d_hid = nt(rows(c0, c1), w2v[blk, :])
        d_pre = (slope * d_hid).astype(BF16)
        da[:, blk] = d_pre
        g = nn(hid, w2v[blk, :])
        g0[...] += g[:half]
        g1[...] += g[half:]
        d = nt(d_pre, w1v[:, blk])
        d0[...] += d[:half]
        d1[...] += d[half:]


def up_body(u0, u1, w1v, h, slope):
    @pl.loop(0, w1v.shape[1] // FB)
    def _(i):
        blk = pl.ds(pl.multiple_of(i * FB, FB), FB)
        hid, s = gelu_pair(nn(rows(u0, u1), w1v[:, blk]))
        h[:, blk] = hid.astype(BF16)
        slope[:, blk] = s


def down_body(base, h, w2v, g0, g1):
    half = g0.shape[0]

    @pl.loop(0, g0.shape[1] // FB)
    def _(i):
        blk = pl.ds(pl.multiple_of(i * FB, FB), FB)
        src = pl.ds(pl.multiple_of(base + i * FB, FB), FB)
        g = nn(h[...], w2v[:, src])
        g0[:, blk] = g[:half]
        g1[:, blk] = g[half:]


def down_back_body(c0, c1, slope, w2v, da):
    @pl.loop(0, w2v.shape[0] // FB)
    def _(i):
        blk = pl.ds(pl.multiple_of(i * FB, FB), FB)
        da[:, blk] = (slope[:, blk] * nt(rows(c0, c1), w2v[blk, :])).astype(BF16)


def up_back_body(base, da, w1v, d0, d1):
    half = d0.shape[0]

    @pl.loop(0, d0.shape[1] // FB)
    def _(i):
        blk = pl.ds(pl.multiple_of(i * FB, FB), FB)
        src = pl.ds(pl.multiple_of(base + i * FB, FB), FB)
        d = nt(da[...], w1v[src, :])
        d0[:, blk] = d[:half]
        d1[:, blk] = d[half:]


def qkv_near_body(u0, u1, w, wo, qkv, wv, wov, sems):
    heads, _, dim, hidden = w.shape
    loads = [pltpu.make_async_copy(w.at[:, j], wv.at[j], sems.at[j]) for j in range(3)]
    loads.append(pltpu.make_async_copy(wo, wov, sems.at[3]))
    for c in loads:
        c.start()
    for j in range(3):
        loads[j].wait()
        qkv[:, j * heads * dim : (j + 1) * heads * dim] = nt(rows(u0, u1), wv[j].reshape(heads * dim, hidden)).astype(BF16)
    loads[3].wait()


def qkv_far_body(u0, u1, wv, qkv):
    _, heads, dim, hidden = wv.shape
    for j in range(3):
        qkv[:, j * heads * dim : (j + 1) * heads * dim] = nt(rows(u0, u1), wv[j].reshape(heads * dim, hidden)).astype(BF16)


GROUP = 256
DIM = 64


def head_mask():
    shape = (GROUP, GROUP)
    return lax.broadcasted_iota(jnp.int32, shape, 0) // DIM == lax.broadcasted_iota(jnp.int32, shape, 1) // DIM


def spread(x, mask):
    tiled = jnp.concatenate([x] * (GROUP // DIM), axis=0)
    return jnp.where(mask, tiled, jnp.zeros_like(tiled))


def fold(x, mask):
    x = jnp.where(mask, x, jnp.zeros_like(x))
    total = x[:DIM]
    for n in range(1, GROUP // DIM):
        total = total + x[n * DIM : (n + 1) * DIM]
    return total


def seg(x, op, ident):
    low = lax.broadcasted_iota(jnp.int32, (x.shape[0], 128), 1) < DIM
    out = []
    for t in range(GROUP // 128):
        xt = x[:, t * 128 : (t + 1) * 128]
        a = op(jnp.where(low, xt, ident), axis=1, keepdims=True)
        b = op(jnp.where(low, ident, xt), axis=1, keepdims=True)
        out.append(jnp.where(low, a, b))
    return jnp.concatenate(out, axis=1)


def pick(near, far, b, col):
    cols = slice(col, col + GROUP)
    return jnp.concatenate([r[s * 64 + b * 16 : s * 64 + b * 16 + 16, cols] for r in (near, far) for s in range(2)], axis=0)


def put(near, far, b, col, x):
    for k, (r, s) in enumerate([(near, 0), (near, 1), (far, 0), (far, 1)]):
        r[s * 64 + b * 16 : s * 64 + b * 16 + 16, col : col + GROUP] = x[k * 16 : k * 16 + 16]


def attn_body(qn, qf, prob, cn, cf):
    width = cn.shape[1]
    mask = head_mask()
    for b in range(4):
        for g in range(width // GROUP):
            col = g * GROUP
            q = pick(qn, qf, b, col)
            k = spread(pick(qn, qf, b, width + col), mask)
            v = spread(pick(qn, qf, b, 2 * width + col), mask)
            s = nt(q, k) * (DIM**-0.5)
            e = jnp.exp(s - seg(s, jnp.max, -jnp.inf))
            p = e / seg(e, jnp.sum, 0.0)
            prob[b * (width // GROUP) + g] = p
            put(cn, cf, b, col, nn(p.astype(BF16), v).astype(BF16))


def attn_back_body(qn, qf, prob, on, of, dn, df):
    width = on.shape[1]
    mask = head_mask()
    for b in range(4):
        for g in range(width // GROUP):
            col = g * GROUP
            q = pick(qn, qf, b, col)
            k = spread(pick(qn, qf, b, width + col), mask)
            v = spread(pick(qn, qf, b, 2 * width + col), mask)
            do = pick(on, of, b, col)
            p = prob[b * (width // GROUP) + g]
            dp = nt(do, v)
            dv = fold(tn(p.astype(BF16), do), mask)
            ds = (p * (dp - seg(dp * p, jnp.sum, 0.0)) * (DIM**-0.5)).astype(BF16)
            dq = nn(ds, k)
            dk = fold(tn(ds, q), mask)
            put(dn, df, b, col, dq.astype(BF16))
            put(dn, df, b, width + col, dk.astype(BF16))
            put(dn, df, b, 2 * width + col, dv.astype(BF16))


def out_body(ctx, wov, f0, f1):
    half = f0.shape[0]

    @pl.loop(0, f0.shape[1] // FB)
    def _(i):
        blk = pl.ds(pl.multiple_of(i * FB, FB), FB)
        f = nn(ctx[...], wov[:, blk])
        f0[:, blk] = f[:half]
        f1[:, blk] = f[half:]


def out_back_body(c0, c1, wov, do):
    @pl.loop(0, wov.shape[0] // FB)
    def _(i):
        blk = pl.ds(pl.multiple_of(i * FB, FB), FB)
        do[:, blk] = nt(rows(c0, c1), wov[blk, :]).astype(BF16)


def qkv_back_body(base, dqkv, wv, d0, d1):
    half = d0.shape[0]
    depth = wv.shape[0] * wv.shape[1] * wv.shape[2]

    @pl.loop(0, d0.shape[1] // FB)
    def _(i):
        blk = pl.ds(pl.multiple_of(i * FB, FB), FB)
        src = pl.ds(pl.multiple_of(base + i * FB, FB), FB)
        d = nn(dqkv[...], wv[:, :, :, src].reshape(depth, FB))
        d0[:, blk] = d[:half]
        d1[:, blk] = d[half:]


def wgrad_body(n_left, *refs):
    left = jnp.concatenate([r[...] for r in refs[:n_left]], axis=0)
    right = jnp.concatenate([r[...] for r in refs[n_left:-1]], axis=0)
    out = refs[-1]
    out[...] = tn(left, right).reshape(out.shape)


def wgrad(left, right, name, block=256):
    n_rows, width = left[0].shape[1], right[0].shape[1]
    return call(
        functools.partial(wgrad_body, len(left)),
        sds((n_rows, width), F32),
        (*left, *right),
        grid=(n_rows // block,),
        in_specs=[pl.BlockSpec((a.shape[0], block), lambda i: (0, i)) for a in left]
        + [pl.BlockSpec(a.shape, lambda i: (0, 0)) for a in right],
        out_specs=pl.BlockSpec((block, width), lambda i: (i, 0)),
        vmem=16,
        flops=2 * 256 * n_rows * width,
        name=name,
    )


def wgrad_qkv(left, right, heads, name):
    per, hidden = 4, right[0].shape[1]
    return call(
        functools.partial(wgrad_body, len(left)),
        sds((heads, 3, DIM, hidden), F32),
        (*left, *right),
        grid=(3, heads // per),
        in_specs=[pl.BlockSpec((a.shape[0], per * DIM), lambda j, i: (0, j * (heads // per) + i)) for a in left]
        + [pl.BlockSpec(a.shape, lambda j, i: (0, 0)) for a in right],
        out_specs=pl.BlockSpec((per, 1, DIM, hidden), lambda j, i: (i, j, 0, 0)),
        vmem=16,
        flops=2 * 256 * heads * 3 * DIM * hidden,
        name=name,
    )


def near_hop(x):
    return lax.ppermute(x, "tp", [(i, i ^ 1) for i in range(4)])


def far_hop(x):
    return lax.ppermute(x, "tp", [(i, i ^ 2) for i in range(4)])


def spread_rows(x):
    far = far_hop(x)
    return x, near_hop(x), far, near_hop(far)


def far_sum(f, d, name):
    total = call(add_body, sds(f.shape, F32), (f, near_hop(d)), vmem=8, flops=f.size, name=name)
    return far_hop(total)


def step(y_one, y_two, dy_one, dy_two, w_qkv, w_out, w_up, w_down):
    state = y_one.shape
    n, hidden = state[0] * state[1], state[2]
    y1, y2, dy1, dy2 = (a.reshape(n, hidden) for a in (y_one, y_two, dy_one, dy_two))
    w1, w2 = w_up[0], w_down[0]
    ffn = w1.shape[1]
    heads, dim = w_qkv.shape[2], w_qkv.shape[4]
    width = heads * dim
    wq = w_qkv[0].transpose(1, 2, 3, 0)
    wo = w_out[0].reshape(width, hidden)
    blk32, blk16 = sds((n, hidden), F32), sds((n, hidden), BF16)
    half32 = sds((n, hidden // 2), F32)
    bulk = 2 * 2 * n * hidden

    u = call(norm_body, blk16, (y1,), vmem=8, flops=4 * n * hidden, name="norm")
    u_me, u_p, u_f, u_d = spread_rows(u)
    c = call(cast_body, blk16, (dy2,), vmem=8, flops=n * hidden, name="cast")
    c_me, c_p, c_f, c_d = spread_rows(c)

    h_n, da_n, g_me, g_p, d_me, d_p, w1v, w2v = call(
        mlp_near_body,
        (sds((2 * n, ffn), BF16), sds((2 * n, ffn), BF16), blk32, blk32, blk32, blk32,
         pltpu.VMEM(w1.shape, BF16), pltpu.VMEM(w2.shape, BF16)),
        (u_me, u_p, c_me, c_p, w1, w2),
        in_specs=[WHOLE] * 4 + [ANY] * 2,
        out_specs=[WHOLE] * 8,
        scratch_shapes=[pltpu.SemaphoreType.DMA((ffn // FB,)), pltpu.SemaphoreType.DMA((ffn // FB,))],
        vmem=36, flops=4 * bulk * ffn, name="mlp_near",
    )
    g_near, d_near = near_hop(g_p), near_hop(d_p)

    h_f, slope = call(up_body, (sds((2 * n, ffn), BF16), sds((2 * n, ffn), F32)), (u_f, u_d, w1v),
                      in_specs=[WHOLE] * 3, out_specs=[WHOLE] * 2, vmem=16, flops=bulk * ffn, name="up_far")
    g_far = []
    for k in range(2):
        gf, gd = call(functools.partial(down_body, k * hidden // 2), (half32, half32), (h_f, w2v),
                      in_specs=[WHOLE] * 2, out_specs=[WHOLE] * 2, vmem=16, flops=bulk * ffn // 2, name=f"down_far{k}")
        g_far.append(far_sum(gf, gd, f"g_sum{k}"))
    da_f = call(down_back_body, sds((2 * n, ffn), BF16), (c_f, c_d, slope, w2v),
                in_specs=[WHOLE] * 4, out_specs=WHOLE, vmem=16, flops=bulk * ffn, name="down_back")
    d_far = []
    for k in range(2):
        df, dd = call(functools.partial(up_back_body, k * hidden // 2), (half32, half32), (da_f, w1v),
                      in_specs=[WHOLE] * 2, out_specs=[WHOLE] * 2, vmem=16, flops=bulk * ffn // 2, name=f"up_back{k}")
        d_far.append(far_sum(df, dd, f"d_sum{k}"))

    dw_down = wgrad((h_n, h_f), (c_me, c_p, c_f, c_d), "dw_down")
    dw_up = wgrad((u_me, u_p, u_f, u_d), (da_n, da_f), "dw_up")

    x2, ua = call(x2_body, (blk32, blk16), (y2, g_me, g_near, *g_far), vmem=16, flops=8 * n * hidden, name="x2")
    a_me, a_p, a_f, a_d = spread_rows(ua)
    qkv_n, wv, wov = call(
        qkv_near_body,
        (sds((2 * n, 3 * width), BF16), pltpu.VMEM((3, heads, dim, hidden), BF16), pltpu.VMEM((width, hidden), BF16)),
        (a_me, a_p, wq, wo), in_specs=[WHOLE] * 2 + [ANY] * 2, out_specs=[WHOLE] * 3,
        scratch_shapes=[pltpu.SemaphoreType.DMA((4,))], vmem=24, flops=bulk * 3 * width, name="qkv_near",
    )
    qkv_f = call(qkv_far_body, sds((2 * n, 3 * width), BF16), (a_f, a_d, wv), in_specs=[WHOLE] * 3, out_specs=WHOLE,
                 vmem=16, flops=bulk * 3 * width, name="qkv_far")
    prob, ctx_n, ctx_f = call(
        attn_body, (sds((4 * width // GROUP, DIM, GROUP), F32), sds((2 * n, width), BF16), sds((2 * n, width), BF16)),
        (qkv_n, qkv_f), in_specs=[WHOLE] * 2, out_specs=[WHOLE] * 3, vmem=16, flops=4e9, name="attn",
    )

    dx1, ca = call(dy_body, (blk32, blk16), (y1, dy1, d_me, d_near, *d_far), vmem=16, flops=8 * n * hidden, name="dy1")
    ca_me, ca_p, ca_f, ca_d = spread_rows(ca)

    f_f, f_d = call(out_body, (blk32, blk32), (ctx_f, wov), in_specs=[WHOLE] * 2, out_specs=[WHOLE] * 2, vmem=16,
                    flops=bulk * width, name="out_far")
    f_me, f_p = call(out_body, (blk32, blk32), (ctx_n, wov), in_specs=[WHOLE] * 2, out_specs=[WHOLE] * 2, vmem=16,
                     flops=bulk * width, name="out_near")
    f_near = near_hop(f_p)
    f_sum = call(add_body, blk32, (f_f, near_hop(f_d)), vmem=8, flops=n * hidden, name="f_sum")
    f_far = [far_hop(f_sum[:, k * hidden // 2 : (k + 1) * hidden // 2]) for k in range(2)]
    x1 = call(sub_body, blk32, (y1, f_me, f_near, *f_far), vmem=16, flops=4 * n * hidden, name="x1")

    do_n = call(out_back_body, sds((2 * n, width), BF16), (ca_me, ca_p, wov), in_specs=[WHOLE] * 3, out_specs=WHOLE,
                vmem=16, flops=bulk * width, name="do_near")
    do_f = call(out_back_body, sds((2 * n, width), BF16), (ca_f, ca_d, wov), in_specs=[WHOLE] * 3, out_specs=WHOLE,
                vmem=16, flops=bulk * width, name="do_far")
    dq_n, dq_f = call(
        attn_back_body, (sds((2 * n, 3 * width), BF16), sds((2 * n, 3 * width), BF16)), (qkv_n, qkv_f, prob, do_n, do_f),
        in_specs=[WHOLE] * 5, out_specs=[WHOLE] * 2, vmem=16, flops=8e9, name="attn_back",
    )
    a_far = []
    for k in range(2):
        af, ad = call(functools.partial(qkv_back_body, k * hidden // 2), (half32, half32), (dq_f, wv),
                      in_specs=[WHOLE] * 2, out_specs=[WHOLE] * 2, vmem=16, flops=bulk * 3 * width // 2, name=f"qkv_back{k}")
        a_far.append(far_sum(af, ad, f"a_sum{k}"))
    a_own, a_oth = call(functools.partial(qkv_back_body, 0), (blk32, blk32), (dq_n, wv), in_specs=[WHOLE] * 2,
                        out_specs=[WHOLE] * 2, vmem=16, flops=bulk * 3 * width, name="qkv_back_near")
    a_near = near_hop(a_oth)
    dw_out = wgrad((ctx_n, ctx_f), (ca_me, ca_p, ca_f, ca_d), "dw_out")
    dw_qkv = wgrad_qkv((dq_n, dq_f), (a_me, a_p, a_f, a_d), heads, "dw_qkv")
    dx2 = call(dx_body, blk32, (x2, dy2, a_own, a_near, *a_far), vmem=16, flops=8 * n * hidden, name="dx2")

    return (
        x1.reshape(state), x2.reshape(state), dx1.reshape(state), dx2.reshape(state),
        dw_qkv.transpose(3, 0, 1, 2)[None], dw_out.reshape(w_out.shape), dw_up[None], dw_down[None],
    )


def solution(mesh):
    state = P("dp", "tp", None)
    return jax.shard_map(
        step,
        mesh=mesh,
        in_specs=(state,) * 4 + (P(None, None, "tp", None, None), P(None, "tp", None, None), P(None, None, "tp"), P(None, "tp", None)),
        out_specs=(state,) * 4 + (P("dp", None, "tp", None, None), P("dp", "tp", None, None), P("dp", None, "tp"), P("dp", "tp", None)),
        check_vma=False,
    )
```
